32 devices in a mesh: gx: 4 (over x, core), gy: 4 (over z), gz: 2 (over y).
Axes of the slice: x: 2, y: 2, z: 4, core: 2. Of those that a mesh axis runs over, the one named last changes fastest.
Arguments:
- hidden_rows: bfloat16 [2048, 16384], P(('gx', 'gy'), 'gz'), may hold values from -2000 to 2000
- norm_gain: bfloat16 [16384], P('gz'), may hold values from 0.5 to 1.5
- w_query: bfloat16 [16384, 16384], P('gz', ('gx', 'gy')), may hold values from -0.046875 to 0.046875
- w_keyval: bfloat16 [16384, 2048], P('gz', ('gx', 'gy')), may hold values from -0.046875 to 0.046875
- positions: int32 [2048], P('gz'), may hold values from 0 to 511, as said below
- keyval_order: int32 [8], replicated, may hold values from 0 to 7, each once
Outputs:
- queries: bfloat16 [2048, 16384], P('gz', ('gx', 'gy'))
- keyval_owned: bfloat16 [8, 2048, 256], P('gy', 'gz')
The draws below stay inside these ranges and needn't reach their ends.
Inputs may be any that keep to these rules, and one draw needn't show every extreme that they name: `positions`: each token's position within its packed document: 0 where a document starts, else one more than the previous token's; a document holds at most 512 tokens. `keyval_order`: each head once.
All inputs are finite; a program needn't handle non-finite values.
Results may differ from the reference program's by a relative error of at most 0.0066.
Values may be sent and summed in bfloat16 or wider, within the bound.
A program may use at most 128 MiB of HBM per device.

```python
import math
import jax
import jax.numpy as jnp
from jax import lax

D = 16384
HQ = 128
KVH = 8
HD = 128
TOKENS = 2048


def draw_hidden_rows(key, part):
    key_rows, key_cols, key_base = jax.random.split(key, 3)
    row_scale = jnp.exp(jax.random.uniform(key_rows, (TOKENS, 1), jnp.float32, 0.0, math.log(10.0)))
    col_place = jnp.arange(D, dtype=jnp.float32) / D
    col_scale = jnp.exp(math.log(3.0) * col_place + jax.random.uniform(key_cols, (D,), jnp.float32, 0.0, math.log(10.0)))
    base_values = jnp.clip(jax.random.normal(key_base, (TOKENS, D), jnp.float32), -6.0, 6.0)
    scaled_values = jnp.clip(base_values * row_scale * col_scale[None, :], -2000.0, 2000.0)
    return scaled_values.astype(jnp.bfloat16)


def draw_positions(key, part):
    longest = TOKENS // 4
    spacing = min(512, max(4, longest // 2))
    marks = jax.random.randint(key, (TOKENS,), 0, spacing)
    index_all = jnp.arange(TOKENS, dtype=jnp.int32)
    is_start = (marks == 0) & (index_all >= longest) | (index_all % longest == 0)
    starts = jnp.where(is_start, index_all, 0)
    return (index_all - lax.cummax(starts, axis=0)).astype(jnp.int32)


def level_of(stream_key, shape, pieces, least, largest):
    def one(dim, blocks):
        draws = jax.random.uniform(jax.random.fold_in(jax.random.fold_in(stream_key, 6), dim), (blocks,), jnp.float32, least / len(pieces), largest / len(pieces))
        return jnp.repeat(jnp.exp(draws), shape[dim] // blocks).reshape((-1,) + (1,) * (len(shape) - dim - 1))

    factor_of = one(*pieces[0])
    for cut in pieces[1:]:
        factor_of = factor_of * one(*cut)
    return factor_of


def normal_values(stream_key, dims, deviation, limit, cuts=(), kind=jnp.bfloat16):
    entries = deviation * jax.random.normal(stream_key, dims, jnp.float32)
    if cuts:
        entries = entries * level_of(stream_key, dims, cuts, -0.22, 0.18)
    return jnp.clip(entries, -limit, limit).astype(kind)


def setup_inputs(seed: int = 0) -> dict:
    key_of = jax.random.split(jax.random.key(seed), 7)
    hidden_rows = draw_hidden_rows(jax.random.fold_in(key_of[6], 71), 0)
    norm_gain = jnp.clip(1.0 + 0.1 * jax.random.normal(key_of[1], (D,), jnp.float32), 0.5, 1.5).astype(jnp.bfloat16)
    w_query = normal_values(key_of[2], (D, HQ * HD), D ** -0.5, 0.046875, ((0, 2), (1, 16)))
    w_keyval = normal_values(key_of[3], (D, 2 * KVH * HD), D ** -0.5, 0.046875, ((0, 2), (1, 16)))
    positions = draw_positions(jax.random.fold_in(key_of[6], 71), 0)
    keyval_order = jax.random.permutation(key_of[5], KVH).astype(jnp.int32)
    return {"hidden_rows": hidden_rows, "norm_gain": norm_gain, "w_query": w_query, "w_keyval": w_keyval, "positions": positions, "keyval_order": keyval_order}


rope_base = 500000.0
norm_eps = 1e-05

def rotate_heads(values, position_ids):
    pair_index = jnp.arange(HD // 2, dtype=jnp.float32)
    inv_freq = jnp.exp(pair_index * (-2.0 * math.log(rope_base) / HD))
    angles = position_ids.astype(jnp.float32)[:, None] * inv_freq[None, :]
    cosines = jnp.cos(angles)[:, None, :]
    sine_part = jnp.sin(angles)[:, None, :]
    paired = values.reshape(values.shape[0], values.shape[1], HD // 2, 2)
    even_part = paired[..., 0]
    odd_part = paired[..., 1]
    rotated = jnp.stack([even_part * cosines - odd_part * sine_part, even_part * sine_part + odd_part * cosines], axis=-1)
    return rotated.reshape(values.shape)

def reference(hidden_rows, norm_gain, w_query, w_keyval, positions, keyval_order):
    widened = hidden_rows.astype(jnp.float32)
    mean_square = lax.optimization_barrier(jnp.sum(widened * widened, axis=1)) / D
    normed = (widened * lax.rsqrt(mean_square + norm_eps)[:, None] * norm_gain.astype(jnp.float32)).astype(jnp.bfloat16)
    query_raw = jnp.dot(normed, w_query, preferred_element_type=jnp.float32)
    queries = rotate_heads(query_raw.reshape(TOKENS, HQ, HD), positions).reshape(TOKENS, HQ * HD).astype(jnp.bfloat16)
    keyval_raw = jnp.dot(normed, w_keyval, preferred_element_type=jnp.float32).reshape(TOKENS, KVH, 2, HD)
    key_rot = rotate_heads(keyval_raw[:, :, 0, :], positions)
    keyval_rot = jnp.stack([key_rot, keyval_raw[:, :, 1, :]], axis=2).reshape(TOKENS, KVH, 2 * HD).astype(jnp.bfloat16)
    keyval_owned = jnp.transpose(keyval_rot[:, keyval_order, :], (1, 0, 2))
    return (queries, keyval_owned)
```

```python
import functools
import math

import jax
import jax.numpy as jnp
from jax import lax
from jax.experimental import pallas as pl
from jax.experimental.pallas import tpu as pltpu
from jax.sharding import PartitionSpec as P

HD = 128
CHUNKS = 1

rope_base = 500000.0
norm_eps = 1e-05


def swap_pairs(values):
    even = (jnp.arange(values.shape[-1]) % 2 == 0)
    return jnp.where(even, jnp.roll(values, -1, axis=-1), jnp.roll(values, 1, axis=-1))


def tables(position_ids, cols, row_scale, is_key):
    within = cols % HD
    inv_freq = jnp.exp((within // 2).astype(jnp.float32) * (-2.0 * math.log(rope_base) / HD))
    angles = position_ids.astype(jnp.float32)[:, None] * inv_freq[None, :]
    sign = jnp.where(cols % 2 == 0, -1.0, 1.0).astype(jnp.float32)[None, :]
    own = jnp.cos(angles)
    other = jnp.sin(angles) * sign
    if is_key is not None:
        own = jnp.where(is_key[None, :], own, 1.0)
        other = jnp.where(is_key[None, :], other, 0.0)
    return own * row_scale[:, None], other * row_scale[:, None]


def rotate_kernel(count, *refs):
    mine_ref = refs[0]
    got_refs = refs[1 : 1 + count]
    own_ref, other_ref = refs[1 + count], refs[2 + count]
    out_ref = refs[-1]
    groups, rows, width = mine_ref.shape
    for group in range(groups):
        own = own_ref[group, 0]
        other = other_ref[group, 0]
        even = lax.broadcasted_iota(jnp.int32, (rows, HD), 1) % 2 == 0
        for head in range(width // HD):
            cols = slice(head * HD, (head + 1) * HD)
            total = mine_ref[group, :, cols]
            for got in got_refs:
                total = total + got[group, :, cols].astype(jnp.float32)
            swapped = jnp.where(even, pltpu.roll(total, HD - 1, 1), pltpu.roll(total, 1, 1))
            out_ref[group, 0, :, cols] = (total * own + swapped * other).astype(out_ref.dtype)


def rotate_into(out, index, chunks, mine, got, own, other):
    groups, rows, width = mine.shape
    step = 2 if groups % 2 == 0 else 1
    part = pl.BlockSpec((step, rows, width), lambda i: (i, 0, 0))
    table = pl.BlockSpec((step, 1, rows, HD), lambda i: (i, index, 0, 0))
    operands = [mine, *got, own, other]
    specs = [part] * (1 + len(got)) + [table] * 2
    alias = {}
    if out is not None:
        alias = {len(operands): 0}
        operands.append(out)
        specs.append(pl.BlockSpec(memory_space=pl.ANY))
    return pl.pallas_call(
        functools.partial(rotate_kernel, len(got)),
        grid=(groups // step,),
        out_shape=jax.ShapeDtypeStruct((groups, chunks, rows, width), jnp.bfloat16),
        in_specs=specs,
        out_specs=pl.BlockSpec((step, 1, rows, width), lambda i: (i, index, 0, 0)),
        input_output_aliases=alias,
        name="rotate_rows",
        cost_estimate=pl.CostEstimate(
            flops=6 * mine.size, bytes_accessed=8 * mine.size, transcendentals=0
        ),
    )(*operands)


def body(hidden_rows, norm_gain, w_query, w_keyval, positions, keyval_order):
    sums = lax.axis_size("gz")
    me = lax.axis_index("gz")
    holders = lax.axis_size("gx") * lax.axis_size("gy")
    group_size = lax.axis_size("gy")
    rows, depth = hidden_rows.shape
    kv_width = w_keyval.shape[1]
    q_width = w_query.shape[1]
    chunks = CHUNKS
    part = rows // chunks
    groups = holders // sums
    gain = norm_gain.astype(jnp.float32)
    col_index = lax.axis_index("gx") * group_size + lax.axis_index("gy")

    gathered = []
    for c in range(chunks):
        piece = hidden_rows[c * part : (c + 1) * part]
        piece = (piece.astype(jnp.float32) * gain[None, :]).astype(jnp.bfloat16)
        gathered.append(lax.all_gather(piece, ("gx", "gy"), axis=0, tiled=True))

    widened = hidden_rows.astype(jnp.float32)
    squares = lax.all_gather(jnp.sum(widened * widened, axis=1), ("gx", "gy", "gz"), axis=0)
    squares = jnp.sum(squares.reshape(holders, sums, rows), axis=1).reshape(holders * rows)
    tokens = holders * rows // sums
    squares = lax.dynamic_slice_in_dim(squares, me * tokens, tokens, 0)
    factor = lax.rsqrt(squares / (depth * sums) + norm_eps)

    q_own, q_other = tables(positions, jnp.arange(HD, dtype=jnp.int32), factor, None)
    q_own = q_own.reshape(groups, chunks, part, HD)
    q_other = q_other.reshape(groups, chunks, part, HD)
    kv_cols = col_index * kv_width + jnp.arange(kv_width, dtype=jnp.int32)
    kv_own, kv_other = tables(positions, kv_cols, factor, kv_cols // HD % 2 == 0)
    kv_own = kv_own.reshape(groups, chunks, part, kv_width)
    kv_other = kv_other.reshape(groups, chunks, part, kv_width)

    def shifts(k):
        return [(i, (i + k) % sums) for i in range(sums)]

    def segment(block, k):
        size = groups * part
        return lax.dynamic_slice_in_dim(block, lax.rem(me + k, sums) * size, size, 0)

    out = None
    keyvals = []
    for c in range(chunks):
        block = gathered[c]
        kv_all = jnp.dot(block, w_keyval, preferred_element_type=jnp.float32)
        kv = segment(kv_all, 0)
        for k in range(1, sums):
            sent = segment(kv_all, k).astype(jnp.bfloat16)
            kv = kv + lax.ppermute(sent, "gz", shifts(k)).astype(jnp.float32)
        kv = kv.reshape(groups, part, kv_width)
        kv = (kv * kv_own[:, c] + swap_pairs(kv) * kv_other[:, c]).astype(jnp.bfloat16)
        keyvals.append(kv)

        got = []
        for k in range(1, sums):
            sent = jnp.dot(
                segment(block, k), w_query, preferred_element_type=jnp.float32
            ).astype(jnp.bfloat16)
            got.append(lax.ppermute(sent, "gz", shifts(k)).reshape(groups, part, q_width))
        mine = jnp.dot(segment(block, 0), w_query, preferred_element_type=jnp.float32)
        mine = mine.reshape(groups, part, q_width)
        out = rotate_into(out, c, chunks, mine, got, q_own, q_other)
    queries = out.reshape(tokens, q_width)

    slot_count = keyval_order.shape[0] // group_size
    wanted = lax.dynamic_slice_in_dim(
        keyval_order, lax.axis_index("gy") * slot_count, slot_count, 0
    )
    half = chunks // 2
    owned = []
    for some in filter(len, (keyvals[:half], keyvals[half:])):
        stacked = jnp.stack(some, axis=1)
        full = lax.all_gather(stacked, ("gx", "gy"), axis=0)
        full = full.reshape(keyval_order.shape[0], -1, *stacked.shape)
        picked = jnp.stack(
            [lax.dynamic_index_in_dim(full, wanted[s], 0, False) for s in range(slot_count)]
        )
        picked = jnp.moveaxis(picked, 1, -2)
        owned.append(picked.reshape(*picked.shape[:-2], -1))
    keyval_owned = jnp.concatenate(owned, axis=2).reshape(slot_count, tokens, 2 * HD)
    return (queries, keyval_owned)


def solution(mesh):
    in_specs = (
        P(("gx", "gy"), "gz"),
        P("gz"),
        P("gz", ("gx", "gy")),
        P("gz", ("gx", "gy")),
        P("gz"),
        P(),
    )
    out_specs = (P("gz", ("gx", "gy")), P("gy", "gz", None))
    return jax.shard_map(body, mesh=mesh, in_specs=in_specs, out_specs=out_specs, check_vma=False)
```
